32 devices in a mesh: patch: 8 (over z, x), rep: 4 (over y, core).
Axes of the slice: x: 2, y: 2, z: 4, core: 2. Of those that a mesh axis runs over, the one named last changes fastest.
Arguments:
- node_latents: bfloat16 [4, 3072, 512], P('rep', 'patch'), may hold values from -6 to 6
- edge_latents: bfloat16 [4, 10240, 512], P('rep', 'patch'), may hold values from -6 to 6
- targets: bfloat16 [4, 3072, 128], P('rep', 'patch'), may hold values from -6 to 6
- edge_weight_in: bfloat16 [1536, 512], replicated, may hold values from -0.15625 to 0.15625
- edge_weight_out: bfloat16 [512, 512], replicated, may hold values from -0.25 to 0.25
- node_weight_in: bfloat16 [1024, 512], replicated, may hold values from -0.1875 to 0.1875
- node_weight_out: bfloat16 [512, 512], replicated, may hold values from -0.25 to 0.25
- readout_weight: bfloat16 [512, 128], replicated, may hold values from -0.25 to 0.25
- send_rows: int32 [8, 96], P('patch'), may hold values from 0 to 383, as said below
- far_rows: int32 [8, 8], P('patch'), may hold values from 0 to 383, as said below
- edge_sender: int32 [10240], P('patch'), may hold values from 0 to 487
- edge_receiver: int32 [10240], P('patch'), may hold values from 0 to 383
- edge_count: int32 [8], P('patch'), may hold values from 80 to 1280, as said below
- land_mask: int32 [3072], P('patch'), may hold values 0 or 1
- lat_band: int32 [3072], P('patch'), may hold values from 0 to 720
Outputs:
- node_grad: bfloat16 [4, 3072, 512], P('rep', 'patch')
- edge_grad: bfloat16 [4, 10240, 512], P('rep', 'patch')
- grad_edge_in: float32 [1536, 512], P('patch')
- grad_edge_out: float32 [512, 512], P('patch')
- grad_node_in: float32 [1024, 512], P('patch')
- grad_node_out: float32 [512, 512], P('patch')
- grad_readout: float32 [512, 128], P('patch')
The draws below stay inside these ranges and needn't reach their ends.
Inputs may be any that keep to these rules, and one draw needn't show every extreme that they name: `send_rows`: the 16 entries of a patch for one neighbour are distinct. `far_rows`: each patch sends exactly one node to every patch (itself included). `edge_count`: some patch has all 1280 edges live.
All inputs are finite; a program needn't handle non-finite values. No bound on the sum of `land_mask` on one device may be relied on, other than what follows from the above.
Results may differ from the reference program's by a relative error of at most 0.012.
Values may be sent and summed in bfloat16 or wider, within the bound.
A program may use at most 128 MiB of HBM per device.

```python
import jax
import jax.numpy as jnp
from jax import lax

D = 512
VARS = 128
OCEAN = 32
BANDS = 721
NODE_DEV = 384
EDGE_DEV = 1280
SLOT = 16
FAR = 1
PATCHES = 8
REPS = 4
NODES = 3072
EDGES = 10240


def draw_send_rows(key, part):
    patches = EDGES // EDGE_DEV
    scores = jax.random.randint(key, (patches, 6, NODE_DEV), 0, 1 << 16) * NODE_DEV + jnp.arange(NODE_DEV, dtype=jnp.int32)
    order = jnp.argsort(scores, axis=-1, stable=True)[:, :, :SLOT]
    return order.reshape(patches, 6 * SLOT).astype(jnp.int32)


def draw_far_rows(key, part):
    patches = EDGES // EDGE_DEV
    scores = jax.random.randint(key, (patches, patches, NODE_DEV), 0, 1 << 16) * NODE_DEV + jnp.arange(NODE_DEV, dtype=jnp.int32)
    order = jnp.argsort(scores, axis=-1, stable=True)[:, :, :FAR]
    return order.reshape(patches, patches * FAR).astype(jnp.int32)


def draw_edge_sender(key, part):
    patches = EDGES // EDGE_DEV
    kind = jax.random.randint(jax.random.fold_in(key, 1), (EDGES,), 0, 100)
    local = jax.random.randint(jax.random.fold_in(key, 2), (EDGES,), 0, NODE_DEV)
    near = NODE_DEV + jax.random.randint(jax.random.fold_in(key, 3), (EDGES,), 0, 6 * SLOT)
    far = NODE_DEV + 6 * SLOT + jax.random.randint(jax.random.fold_in(key, 4), (EDGES,), 0, FAR * patches)
    return jnp.where(kind < 72, local, jnp.where(kind < 88, near, far)).astype(jnp.int32)


def draw_edge_count(key, part):
    patches = EDGES // EDGE_DEV
    counts = jax.random.randint(key, (patches,), EDGE_DEV // 16, EDGE_DEV + 1)
    fullest = jax.random.randint(jax.random.fold_in(key, 7), (), 0, patches)
    return jnp.where(jnp.arange(patches) == fullest, EDGE_DEV, counts).astype(jnp.int32)


def with_ends(entries, own_key, least, high):
    dims = entries.shape
    spot = [jax.random.randint(jax.random.fold_in(own_key, axis), (), 0, dims[axis]) for axis in range(len(dims))]
    entries = entries.at[tuple(spot)].set(least)
    longest = dims.index(max(dims))
    spot[longest] = (spot[longest] + 1) % dims[longest]
    return entries.at[tuple(spot)].set(high)


def block_levels(rng, extent, pieces, low, high):
    def one(position, parts):
        draws = jax.random.uniform(jax.random.fold_in(jax.random.fold_in(rng, 6), position), (parts,), jnp.float32, low / len(pieces), high / len(pieces))
        return jnp.repeat(jnp.exp(draws), extent[position] // parts).reshape((-1,) + (1,) * (len(extent) - position - 1))

    factor_of = one(*pieces[0])
    for cut in pieces[1:]:
        factor_of = factor_of * one(*cut)
    return factor_of


def normal_values(stream_key, dims, scale, most, split=(), kind=jnp.bfloat16):
    entries = scale * jax.random.normal(stream_key, dims, jnp.float32)
    if split:
        entries = entries * block_levels(stream_key, dims, split, -0.22, 0.18)
    return jnp.clip(entries, -most, most).astype(kind)


def setup_inputs(seed: int = 0) -> dict:
    key_of = jax.random.split(jax.random.key(seed), 16)
    node_latents = normal_values(key_of[0], (REPS, NODES, D), 1.0, 6.0, ((0, 4), (1, 8)))
    edge_latents = normal_values(key_of[1], (REPS, EDGES, D), 1.0, 6.0, ((0, 4), (1, 8)))
    targets = normal_values(key_of[2], (REPS, NODES, VARS), 1.0, 6.0, ((0, 4), (1, 8)))
    edge_weight_in = normal_values(key_of[3], (3 * D, D), (3 * D) ** -0.5, 0.15625)
    edge_weight_out = normal_values(key_of[4], (D, D), D ** -0.5, 0.25)
    node_weight_in = normal_values(key_of[5], (2 * D, D), (2 * D) ** -0.5, 0.1875)
    node_weight_out = normal_values(key_of[6], (D, D), D ** -0.5, 0.25)
    readout_weight = normal_values(key_of[7], (D, VARS), D ** -0.5, 0.25)
    send_rows = draw_send_rows(jax.random.fold_in(key_of[15], 71), 0)
    far_rows = draw_far_rows(jax.random.fold_in(key_of[15], 71), 0)
    edge_sender = draw_edge_sender(jax.random.fold_in(key_of[15], 71), 0)
    edge_receiver = with_ends(jax.random.randint(key_of[11], (EDGES,), 0, NODE_DEV), jax.random.fold_in(key_of[11], 1), 0, NODE_DEV - 1).astype(jnp.int32)
    edge_count = draw_edge_count(jax.random.fold_in(key_of[15], 71), 0)
    land_mask = with_ends((jax.random.randint(key_of[13], (NODES,), 0, 10) < 3).astype(jnp.int32), jax.random.fold_in(key_of[13], 1), 0, 1)
    lat_band = with_ends(jax.random.randint(key_of[14], (NODES,), 0, BANDS), jax.random.fold_in(key_of[14], 1), 0, BANDS - 1).astype(jnp.int32)
    return {"node_latents": node_latents, "edge_latents": edge_latents, "targets": targets, "edge_weight_in": edge_weight_in, "edge_weight_out": edge_weight_out, "node_weight_in": node_weight_in, "node_weight_out": node_weight_out, "readout_weight": readout_weight, "send_rows": send_rows, "far_rows": far_rows, "edge_sender": edge_sender, "edge_receiver": edge_receiver, "edge_count": edge_count, "land_mask": land_mask, "lat_band": lat_band}


def normalize(values):
    average = lax.optimization_barrier(jnp.mean(values, axis=-1, keepdims=True))
    centred = values - average
    variance = lax.optimization_barrier(jnp.mean(centred * centred, axis=-1, keepdims=True))
    inverse = lax.rsqrt(variance + 1e-05)
    return (centred * inverse, inverse)

def norm_back(gradient, normed, inverse):
    first = lax.optimization_barrier(jnp.mean(gradient, axis=-1, keepdims=True))
    second = lax.optimization_barrier(jnp.mean(gradient * normed, axis=-1, keepdims=True))
    return inverse * (gradient - first - normed * second)

def silu_grad(values):
    logistic = jax.nn.sigmoid(values)
    return logistic * (1.0 + values * (1.0 - logistic))

def product(left, right):
    return jnp.dot(left, right, preferred_element_type=jnp.float32)

def product_left(left, right):
    return jnp.dot(left.T, right, preferred_element_type=jnp.float32)

def product_right(left, right):
    return jnp.dot(left, right.T, preferred_element_type=jnp.float32)

def reference(node_latents, edge_latents, targets, edge_weight_in, edge_weight_out, node_weight_in, node_weight_out, readout_weight, send_rows, far_rows, edge_sender, edge_receiver, edge_count, land_mask, lat_band):
    positions = jnp.arange(EDGES, dtype=jnp.int32)
    device = (positions // EDGE_DEV).astype(jnp.int32)
    near_total = 6 * SLOT
    offset = jnp.maximum(edge_sender - NODE_DEV, 0).astype(jnp.int32)
    near_index = jnp.minimum(offset, near_total - 1).astype(jnp.int32)
    neighbour = (near_index // SLOT).astype(jnp.int32)
    distance = ((neighbour // 2 + 1) * (1 - 2 * (neighbour % 2))).astype(jnp.int32)
    near_patch = ((device - distance + PATCHES) % PATCHES).astype(jnp.int32)
    near_node = near_patch * NODE_DEV + send_rows[near_patch, near_index]
    far_index = jnp.maximum(offset - near_total, 0).astype(jnp.int32)
    far_patch = jnp.minimum(far_index // FAR, PATCHES - 1).astype(jnp.int32)
    far_node = far_patch * NODE_DEV + far_rows[far_patch, device * FAR + far_index % FAR]
    remote = jnp.where(offset < near_total, near_node, far_node)
    senders = jnp.where(edge_sender < NODE_DEV, device * NODE_DEV + edge_sender, remote).astype(jnp.int32)
    receivers = (device * NODE_DEV + edge_receiver).astype(jnp.int32)
    alive_mask = (positions % EDGE_DEV < edge_count[device]).astype(jnp.float32)[:, None]
    latitude = -0.5 * jnp.pi + (lat_band.astype(jnp.float32) + 0.5) * (jnp.pi / BANDS)
    area_weight = jnp.cos(latitude)[:, None]
    channel = jnp.arange(VARS, dtype=jnp.int32)
    keep_mask = jnp.where((channel[None, :] < OCEAN) & (land_mask[:, None] == 1), 0.0, 1.0).astype(jnp.float32)
    loss_weight = area_weight * keep_mask
    sums = [jnp.zeros(w.shape, jnp.float32) for w in (edge_weight_in, edge_weight_out, node_weight_in, node_weight_out, readout_weight)]
    node_grads = []
    edge_grads = []
    for replica in range(REPS):
        node_rows = node_latents[replica]
        edge_rows = edge_latents[replica]
        stacked = jnp.concatenate([node_rows[senders], node_rows[receivers], edge_rows], axis=1)
        edge_pre = product(stacked, edge_weight_in)
        edge_hidden = jax.nn.silu(edge_pre).astype(jnp.bfloat16)
        edge_normed, edge_inverse = normalize(product(edge_hidden, edge_weight_out))
        message = (edge_normed * alive_mask).astype(jnp.bfloat16)
        aggregate = jax.ops.segment_sum(message.astype(jnp.float32), receivers, num_segments=NODES).astype(jnp.bfloat16)
        node_input = jnp.concatenate([node_rows, aggregate], axis=1)
        node_pre = product(node_input, node_weight_in)
        node_hidden = jax.nn.silu(node_pre).astype(jnp.bfloat16)
        node_normed, node_inverse = normalize(product(node_hidden, node_weight_out))
        updated = (node_rows.astype(jnp.float32) + node_normed).astype(jnp.bfloat16)
        predicted = product(updated, readout_weight)
        pred_grad = (loss_weight * (predicted - targets[replica].astype(jnp.float32))).astype(jnp.bfloat16)
        updated_grad = product_right(pred_grad, readout_weight)
        node_z_grad = norm_back(updated_grad, node_normed, node_inverse).astype(jnp.bfloat16)
        node_pre_grad = (product_right(node_z_grad, node_weight_out) * silu_grad(node_pre)).astype(jnp.bfloat16)
        input_grad = product_right(node_pre_grad, node_weight_in)
        message_grad = input_grad[:, D:][receivers] * alive_mask
        edge_z_grad = norm_back(message_grad, edge_normed, edge_inverse).astype(jnp.bfloat16)
        edge_pre_grad = (product_right(edge_z_grad, edge_weight_out) * silu_grad(edge_pre)).astype(jnp.bfloat16)
        stacked_grad = product_right(edge_pre_grad, edge_weight_in)
        sender_grad = stacked_grad[:, :D].astype(jnp.bfloat16).astype(jnp.float32)
        receiver_grad = stacked_grad[:, D:2 * D].astype(jnp.bfloat16).astype(jnp.float32)
        edge_grads.append(stacked_grad[:, 2 * D:].astype(jnp.bfloat16))
        total = updated_grad + input_grad[:, :D]
        total = total + jax.ops.segment_sum(sender_grad, senders, num_segments=NODES)
        total = total + jax.ops.segment_sum(receiver_grad, receivers, num_segments=NODES)
        node_grads.append(total.astype(jnp.bfloat16))
        sums[0] = sums[0] + product_left(stacked, edge_pre_grad)
        sums[1] = sums[1] + product_left(edge_hidden, edge_z_grad)
        sums[2] = sums[2] + product_left(node_input, node_pre_grad)
        sums[3] = sums[3] + product_left(node_hidden, node_z_grad)
        sums[4] = sums[4] + product_left(updated, pred_grad)
    factor = 1.0 / (NODES * REPS)
    return (jnp.stack(node_grads), jnp.stack(edge_grads), sums[0] * factor, sums[1] * factor, sums[2] * factor, sums[3] * factor, sums[4] * factor)
```

```python
import functools

import jax
import jax.numpy as jnp
from jax import lax
from jax.experimental import pallas as pl
from jax.experimental.pallas import tpu as pltpu
from jax.sharding import PartitionSpec as P

OCEAN = 32
BANDS = 721
OFFSETS = (1, -1, 2, -2, 3, -3)
MESH = pl.DeviceIdType.MESH
F32 = jnp.float32
BF16 = jnp.bfloat16


def mm(left, right):
    return jnp.dot(left, right, preferred_element_type=F32)


def mm_left(left, right):
    return lax.dot_general(left, right, (((0,), (0,)), ((), ())), preferred_element_type=F32)


def mm_right(left, right):
    return lax.dot_general(left, right, (((1,), (1,)), ((), ())), preferred_element_type=F32)


def logistic(values):
    return 0.5 * jnp.tanh(0.5 * values) + 0.5


def mean(values):
    return jnp.mean(values, axis=-1, keepdims=True)


def parse(kind):
    order = ("side",) + tuple(AXES[letter] for letter in kind if letter in AXES)
    return order, "W" in kind, "+" in kind


AXES = {"l": "low", "w": "wide", "h": "high"}


class Stream:
    def __init__(self, refs, kind, sizes, patch, rep):
        self.sizes, self.patch, self.rep = sizes, patch, rep
        self.order, self.sums, self.direct = parse(kind)
        n = len(self.order)
        self.own, self.got, self.acc = refs[0], refs[1 : 1 + n], refs[1 + n : 1 + 2 * n]
        self.last, self.fin, self.send, self.recv = refs[1 + 2 * n :]
        self.at = {"side": lax.rem(rep, 2), "wide": lax.div(rep, 2), "low": lax.rem(patch, 2), "high": lax.div(patch, 2)}
        self.sent, self.wait, self.done = None, None, 0

    def device(self, axis, index):
        at = dict(self.at)
        at[axis] = index
        return (2 * at["high"] + at["low"], 2 * at["wide"] + at["side"])

    def others(self, axis):
        size = self.sizes[axis]
        return [(d, lax.rem(self.at[axis] + d, size)) for d in range(1, size)]

    def peers(self, axis):
        return [self.device(axis, other) for _, other in self.others(axis)]

    def launch(self, ids, pairs, whole):
        if self.sent is not None:
            self.sent()
        copies = []
        for device, (src, dst) in zip(ids, pairs):
            copies.append(pltpu.make_async_remote_copy(
                src_ref=src, dst_ref=dst, send_sem=self.send.at[0], recv_sem=self.recv.at[self.done - 1],
                device_id=device, device_id_type=MESH))
            copies[-1].start()
        if len(copies) == 1:
            self.sent, self.wait = copies[0].wait_send, copies[0].wait_recv
        else:
            self.sent = pltpu.make_async_copy(whole, whole, self.send.at[0]).wait
            self.wait = pltpu.make_async_copy(whole, whole, self.recv.at[self.done - 1]).wait

    def arrive(self):
        if self.wait is not None:
            self.wait()
        self.wait = None

    def total(self, first, rest, count):
        if count == 1:
            return first + rest[0]
        value = first.astype(F32)
        for d in range(count):
            value = value + rest[d].astype(F32)
        return value.astype(BF16)

    def step(self):
        now, stages = self.done, len(self.order)
        self.done += 1
        held = self.own
        self.arrive()
        if 0 < now <= stages:
            axis = self.order[now - 1]
            before = self.own if now == 1 else self.acc[now - 2]
            held = self.acc[now - 1]
            held[...] = self.total(before[self.at[axis]], self.got[now - 1], self.sizes[axis] - 1)
        if now < stages:
            axis = self.order[now]
            pairs = [(held.at[other], self.got[now].at[d - 1]) for d, other in self.others(axis)]
            self.launch(self.peers(axis), pairs, self.got[now])
            return
        side, wide = self.at["side"], self.at["wide"]
        if self.direct:
            self.fin[side, wide] = held[...]
            reps = self.sizes["side"] * self.sizes["wide"]
            ids = [(self.patch, lax.rem(self.rep + d, reps)) for d in range(1, reps)]
            self.launch(ids, [(held, self.fin.at[side, wide])] * (reps - 1), self.last)
            return
        if now == stages:
            if not self.sums:
                self.fin[side, wide] = held[...]
            pairs = [
                (held, self.last.at[d - 1] if self.sums else self.fin.at[side, wide])
                for d, _ in self.others("wide")]
            self.launch(self.peers("wide"), pairs, self.last)
        elif now == stages + 1:
            if self.sums:
                self.fin[side] = self.total(self.acc[-1][...], self.last, self.sizes["wide"] - 1)
            self.launch(self.peers("side"), [(self.fin.at[side], self.fin.at[side])], None)

    def finish(self):
        self.sent()


def stream_scratch(kind, rows, width, sizes):
    order, sums, direct = parse(kind)
    lead = tuple(sizes[a] for a in order)
    scratch = [pltpu.VMEM(lead + (rows, width), BF16)]
    for i, axis in enumerate(order):
        scratch.append(pltpu.VMEM((max(sizes[axis] - 1, 1),) + lead[i + 1 :] + (rows, width), BF16))
    for i in range(len(order)):
        scratch.append(pltpu.VMEM(lead[i + 1 :] + (rows, width), BF16))
    last = sizes["side"] * sizes["wide"] - 1 if direct else max(sizes["wide"] - 1, 1)
    scratch.append(pltpu.VMEM((last, rows, width), BF16))
    fin = (sizes["side"],) if sums and not direct else (sizes["side"], sizes["wide"])
    scratch.append(pltpu.VMEM(fin + (rows, width), BF16))
    return scratch + [pltpu.SemaphoreType.DMA((1,)), pltpu.SemaphoreType.DMA((len(order) + 2,))]


def layout(stream, block):
    rows, width = stream.own.shape[-2:]
    by_row = block["by_row"]
    wides = 1 if stream.sums else stream.sizes["wide"]
    for side in range(2):
        for wide in range(wides):
            low = block["low"] + wide * rows + (side * rows * wides if by_row else 0)
            col = block["col"] + (0 if by_row else side * width)
            yield side, wide, low, col, rows, width


def put(stream, value, block):
    patches = stream.sizes["low"] * stream.sizes["high"]
    height = value.shape[0] // patches
    for p in range(patches):
        for side, wide, low, col, rows, width in layout(stream, block):
            at = {"side": side, "wide": wide, "low": p % 2, "high": p // 2}
            stream.own[tuple(at[a] for a in stream.order) + (slice(None), slice(None))] = value[
                p * height + low : p * height + low + rows, col : col + width
            ].astype(BF16)


def take(stream, out, block, scale, shift=0):
    for side, wide, low, col, rows, width in layout(stream, block):
        if stream.sums and stream.direct:
            held = stream.fin[side, 0].astype(F32)
            for w in range(1, stream.sizes["wide"]):
                held = held + stream.fin[side, w].astype(F32)
        else:
            held = (stream.fin[side] if stream.sums else stream.fin[side, wide]).astype(F32)
        out[low : low + rows, shift + col : shift + col + width] = held * scale


def stream_specs(share, width, variables):
    sides = {
        "ro": (share, variables), "no": (share, width), "ni": (2 * share, width), "eo": (share, width),
        "c0": (3 * share, width // 2), "c1": (3 * share, width // 2)}
    specs = []
    for group, down, across, kinds in STREAMS:
        height, columns = sides[group][0] // down, sides[group][1] // across
        by_row = group == "ro"
        for i, kind in enumerate(kinds):
            rows, cols = (height // 2, columns) if by_row else (height, columns // 2)
            place = {"low": (i // across) * height, "col": (i % across) * columns, "by_row": by_row}
            specs.append((f"{group}_{i}", kind, rows if parse(kind)[1] else rows // 2, cols, place))
    return specs


def kernel(
    dims,
    x_h, e_h, tgt_h, wein_h, weout_h, wnin_h, wnout_h, wro_h, send_h, far_h, es_h, er_h, count_h, land_h, lat_h,
    o_node, o_edge, o_ein, o_eout, o_nin, o_nout, o_ro,
    x, e, tgt, w_ein, w_eout, w_nin, w_nout, w_ro, send_ids, far_ids, es, er, count, land, lat, loaded,
    near_out, near_in, far_out, far_in, back_near_out, back_near_in, back_far_out, back_far_in,
    xext, xw, table, sgrad, hid, msg, inv, ezg, epg, agg_grad, total, sums, rsums, local, loss_weight,
    halo_sems, back_sems,
    *stream_refs,
):
    patches, reps, slot, far, ext, tile = dims
    nodes, width = x.shape
    edges = e.shape[0]
    near = 6 * slot
    share = width // patches
    half = width // 2
    patch, rep = lax.axis_index("patch"), lax.axis_index("rep")
    sizes = {"side": 2, "wide": reps // 2, "low": 2, "high": patches // 2}

    barrier = pltpu.get_barrier_semaphore()
    for d in range(1, patches):
        pl.semaphore_signal(barrier, inc=1, device_id=(lax.rem(patch + d, patches), rep), device_id_type=MESH)
    for d in range(1, reps):
        pl.semaphore_signal(barrier, inc=1, device_id=(patch, lax.rem(rep + d, reps)), device_id_type=MESH)

    loads = {}
    order = ("x", "send", "far", "wein", "er", "es", "count", "e", "weout", "wnin", "wnout", "wro", "tgt", "land", "lat")
    source = dict(
        x=(x_h, x), send=(send_h, send_ids), far=(far_h, far_ids), wein=(wein_h, w_ein), er=(er_h, er), es=(es_h, es),
        count=(count_h, count), e=(e_h, e), weout=(weout_h, w_eout), wnin=(wnin_h, w_nin), wnout=(wnout_h, w_nout),
        wro=(wro_h, w_ro), tgt=(tgt_h, tgt), land=(land_h, land), lat=(lat_h, lat))
    for i, name in enumerate(order):
        loads[name] = pltpu.make_async_copy(source[name][0], source[name][1], loaded.at[i])
        loads[name].start()

    specs = stream_specs(share, width, tgt.shape[1])
    streams, used = [], 0
    for _, kind, _, _, _ in specs:
        refs = 5 + 2 * len(parse(kind)[0])
        streams.append(Stream(stream_refs[used : used + refs], kind, sizes, patch, rep))
        used += refs
    named = {spec[0]: s for s, spec in zip(streams, specs)}
    groups = {}
    for s, spec in zip(streams, specs):
        groups.setdefault(spec[0][:2], []).append((s, spec[4]))

    def put_group(group, value):
        for s, place in groups[group]:
            put(s, value, place)
            s.step()

    returned = []

    def send_back():
        for k in range(6):
            back_near_out[k] = sums[nodes + k * slot : nodes + (k + 1) * slot, :]
        for q in range(patches):
            low = nodes + near + q * far
            back_far_out[q] = sums[low : low + far, :]
        returned.extend(exchange(-1, back_near_out, back_near_in, back_far_out, back_far_in, back_sems))

    def node_out():
        for c in returned[1]:
            c.wait()
        near_back = jnp.concatenate([back_near_in[k] for k in range(6)], axis=0)
        far_back = jnp.concatenate([back_far_in[q].astype(F32) for q in range(patches)], axis=0).astype(BF16)
        owned = mm(own_near, near_back) + mm(own_far, far_back)
        owned = (owned + local[...]).astype(BF16)
        o_node[...] = (total[...] + mm_right(owned, w_s[...])).astype(BF16)

    actions = {"back": send_back, "node": node_out}
    plan = iter(PLAN)

    def tick():
        for name in next(plan):
            if name in actions:
                actions[name]()
                continue
            named[name].step()

    def listed(ids):
        hit = lax.broadcasted_iota(jnp.int32, (nodes, ids.shape[1]), 0) == ids[...]
        return jnp.where(hit, 1.0, 0.0).astype(BF16)

    for name in ("x", "send", "far"):
        loads[name].wait()
    own_near, own_far = listed(send_ids), listed(far_ids)
    outgoing, outgoing_far = mm_left(own_near, x[...]), mm_left(own_far, x[...])
    for k in range(6):
        near_out[k] = outgoing[k * slot : (k + 1) * slot].astype(BF16)
    for q in range(patches):
        far_out[q] = outgoing_far[q * far : (q + 1) * far].astype(BF16)
    pl.semaphore_wait(barrier, patches - 1 + reps - 1)

    def remote(src, dst, send, recv, device):
        c = pltpu.make_async_remote_copy(
            src_ref=src, dst_ref=dst, send_sem=send, recv_sem=recv, device_id=device, device_id_type=MESH)
        c.start()
        return c

    def exchange(sign, near_from, near_to, far_from, far_to, sems):
        near_send, near_recv, far_send, far_recv = (sems.at[i] for i in range(4))
        for d in range(1, patches):
            to = lax.rem(patch + d, patches)
            remote(far_from.at[to], far_to.at[patch], far_send, far_recv, (to, rep))
        for k, o in reversed(tuple(enumerate(OFFSETS))):
            remote(near_from.at[k], near_to.at[k], near_send, near_recv, (lax.rem(patch + (sign * o + patches), patches), rep))
        far_to[patch] = far_from[patch]
        others = far_from.at[pl.ds(0, patches - 1)]
        return (
            [pltpu.make_async_copy(near_from, near_from, near_send), pltpu.make_async_copy(others, others, far_send)],
            [pltpu.make_async_copy(near_to, near_to, near_recv), pltpu.make_async_copy(others, others, far_recv)])

    halo_sent, halo = exchange(1, near_out, near_in, far_out, far_in, halo_sems)

    w_s, w_r, w_e = (w_ein.at[pl.ds(i * width, width)] for i in range(3))
    loads["wein"].wait()
    xext[0:nodes, :] = x[...]
    xw[0:nodes, :] = mm(x[...], w_s[...]).astype(BF16)
    xw[nodes : 2 * nodes, :] = mm(x[...], w_r[...]).astype(BF16)
    own, far_rows = 2 * nodes, ext - nodes

    for name in ("er", "es", "count", "e"):
        loads[name].wait()

    def tables(t):
        at = slice(t * tile, (t + 1) * tile)
        ids = es[at][None, :]
        hit = lax.broadcasted_iota(jnp.int32, (nodes, tile), 0) == ids
        table[0:nodes, at] = jnp.where(hit, 1.0, 0.0).astype(BF16)
        hit = lax.broadcasted_iota(jnp.int32, (far_rows, tile), 0) + nodes == ids
        table[own : own + far_rows, at] = jnp.where(hit, 1.0, 0.0).astype(BF16)
        alive = lax.broadcasted_iota(jnp.int32, (1, tile), 1) + t * tile < count[0]
        ids = jnp.where(alive, er[at][None, :], -1)
        hit = lax.broadcasted_iota(jnp.int32, (nodes, tile), 0) == ids
        table[nodes : 2 * nodes, at] = jnp.where(hit, 1.0, 0.0).astype(BF16)

    def edge_local(t):
        at = slice(t * tile, (t + 1) * tile)
        sgrad[at, :] = mm(e[at, :], w_e[...]) + mm_left(table[0:own, at], xw[0:own, :])

    parts = range(edges // tile)
    for t in parts:
        tables(t)
        edge_local(t)

    for name in order[8:]:
        loads[name].wait()
    variables = tgt.shape[1]
    latitude = -0.5 * jnp.pi + (lat[...].astype(F32) + 0.5) * (jnp.pi / BANDS)
    area = jnp.broadcast_to(jnp.cos(latitude)[None, :], (variables, nodes))
    ocean = lax.broadcasted_iota(jnp.int32, (variables, nodes), 0) < OCEAN
    masked = jnp.broadcast_to((land[...])[None, :], (variables, nodes)) == 1
    loss_weight[...] = jnp.transpose(jnp.where(ocean & masked, 0.0, area))
    total[...] = mm(x[...], w_nin[0:width, :])

    for c in halo:
        c.wait()
    pieces = [near_in[k] for k in range(6)] + [far_in[q] for q in range(patches)]
    pad = ext - nodes - near - patches * far
    if pad:
        pieces.append(jnp.zeros((pad, width), BF16))
    arrived = jnp.concatenate([v.astype(F32) for v in pieces], axis=0).astype(BF16)
    xext[nodes:ext, :] = arrived
    xw[own : own + far_rows, :] = mm(arrived, w_s[...]).astype(BF16)

    def edge_hidden(t):
        at = slice(t * tile, (t + 1) * tile)
        pre = sgrad[at, :] + mm_left(table[own : own + far_rows, at], xw[own : own + far_rows, :])
        s = logistic(pre)
        h = pre * s
        sgrad[at, :] = s + h * (1.0 - s)
        hid[at, :] = h.astype(BF16)

    def edge_normed(t):
        at = slice(t * tile, (t + 1) * tile)
        z = mm(hid[at, :], w_eout[...])
        centred = z - mean(z)
        inverse = lax.rsqrt(mean(centred * centred) + 1e-05)
        inv[at, :] = inverse
        msg[at, :] = (centred * inverse).astype(BF16)

    for t in parts:
        edge_hidden(t)
        edge_normed(t)

    aggregate = mm(table[nodes : 2 * nodes, :], msg[...]).astype(BF16)
    node_pre = total[...] + mm(aggregate, w_nin[width : 2 * width, :])
    s = logistic(node_pre)
    h = node_pre * s
    node_hidden = h.astype(BF16)
    node_sgrad = s + h * (1.0 - s)
    z = mm(node_hidden, w_nout[...])
    centred = z - mean(z)
    inverse = lax.rsqrt(mean(centred * centred) + 1e-05)
    normed = centred * inverse
    updated = (x[...].astype(F32) + normed).astype(BF16)
    pred_grad = (loss_weight[...] * (mm(updated, w_ro[...]) - tgt[...].astype(F32))).astype(BF16)
    up_grad = mm_right(pred_grad, w_ro[...])
    z_grad = (inverse * (up_grad - mean(up_grad) - normed * mean(up_grad * normed))).astype(BF16)
    put_group("no", mm_left(node_hidden, z_grad))
    tick()
    pre_grad = (mm_right(z_grad, w_nout[...]) * node_sgrad).astype(BF16)
    put_group("ni", jnp.concatenate([mm_left(x[...], pre_grad), mm_left(aggregate, pre_grad)], axis=0))
    tick()
    total[...] = up_grad + mm_right(pre_grad, w_nin[0:width, :])
    message_grad = mm_right(pre_grad, w_nin[width : 2 * width, :])
    agg_grad[...] = (message_grad - mean(message_grad)).astype(BF16)
    put_group("ro", mm_left(updated, pred_grad))
    tick()

    def edge_backward(t):
        at = slice(t * edges // 2, (t + 1) * edges // 2)
        g = mm_left(table[nodes : 2 * nodes, at], agg_grad[...])
        y = msg[at, :].astype(F32)
        zg = (inv[at, :] * (g - y * mean(g * y))).astype(BF16)
        ezg[at, :] = zg
        epg[at, :] = (mm_right(zg, w_eout[...]) * sgrad[at, :]).astype(BF16)

    for t in range(2):
        edge_backward(t)
        tick()
    put_group("eo", mm_left(hid[...], ezg[...]))
    tick()

    for c, group in enumerate(("c0", "c1")):
        at = pl.ds(c * half, half)
        sums32 = mm(table[0:nodes, :], epg[:, at])
        local[:, at] = sums32
        sums[0:nodes, at] = sums32.astype(BF16)
        sums[nodes:ext, at] = mm(table[own : own + far_rows, :], epg[:, at]).astype(BF16)
        tick()
        rsums[:, at] = mm(table[nodes : 2 * nodes, :], epg[:, at]).astype(BF16)
        tick()
        first = mm_left(e[...], epg[:, at])
        tick()
        put_group(group, jnp.concatenate(
            [mm_left(xext[...], sums[:, at]), mm_left(x[...], rsums[:, at]), first], axis=0))
        tick()

    for t in range(2):
        at = slice(t * edges // 2, (t + 1) * edges // 2)
        o_edge[at, :] = mm_right(epg[at, :], w_e[...]).astype(BF16)
        tick()
    total[...] += mm_right(rsums[...], w_r[...])
    tick()
    for s in streams:
        assert s.done == len(s.order) + (1 if s.direct else 2)

    scale = 1.0 / (nodes * patches * reps)
    for c in halo_sent + returned[0]:
        c.wait()
    into = {"ro": (o_ro, 0), "no": (o_nout, 0), "ni": (o_nin, 0), "eo": (o_eout, 0), "c0": (o_ein, 0), "c1": (o_ein, half)}
    for group, members in groups.items():
        for s, place in members:
            s.arrive()
            take(s, into[group][0], place, scale, into[group][1])
    for s in streams:
        s.finish()


STREAMS = (
    ("ro", 1, 1, ("wlh",)),
    ("no", 1, 2, ("hlw+", "wlh")),
    ("ni", 1, 2, ("hwl", "lwh+")),
    ("eo", 1, 2, ("wlh+", "lhW")),
    ("c0", 3, 1, ("wlh+", "lhW+", "wlh+")),
    ("c1", 3, 1, ("lwh+", "wlh", "wlh+")),
)


PLAN = (
    (),
    ("no_0",),
    ("no_1",),
    ("ni_0", "ni_1", "ro_0"),
    (),
    ("no_1",),
    ("ro_0",),
    (),
    ("eo_0", "no_0"),
    ("eo_1", "ni_1"),
    (),
    ("no_1", "ro_0", "back"),
    ("c0_0", "no_0", "c0_1", "c0_2"),
    ("eo_0",),
    ("eo_1", "ni_1"),
    ("c1_0", "c1_1", "c1_2", "ni_0"),
    ("c0_0", "no_0", "no_1", "ro_0", "c0_1", "c0_2", "eo_0", "c1_1", "node", "c1_0", "c0_0", "eo_1", "c1_2",
     "c0_2", "ni_0", "ni_1", "c1_1", "no_1", "ro_0", "c1_0", "eo_1", "c0_1", "c1_2", "ni_0", "eo_0", "c0_0",
     "c0_2", "c1_1", "ni_0", "c1_0", "c1_2", "c1_1"),
)


def settle_kernel(n, *refs):
    src, dst, sem = refs[:n], refs[n : 2 * n], refs[2 * n]
    copies = [pltpu.make_async_copy(src[i], dst[i], sem.at[i]) for i in range(n)]
    for c in copies:
        c.start()
    for c in copies:
        c.wait()


def settle(arrays):
    n = len(arrays)
    return pl.pallas_call(
        functools.partial(settle_kernel, n),
        out_shape=tuple(jax.ShapeDtypeStruct(a.shape, a.dtype) for a in arrays),
        in_specs=[pl.BlockSpec(memory_space=pltpu.VMEM)] * n,
        out_specs=tuple([pl.BlockSpec(memory_space=pltpu.HBM)] * n),
        scratch_shapes=[pltpu.SemaphoreType.DMA((n,))],
        compiler_params=pltpu.CompilerParams(vmem_limit_bytes=4 * 1024 * 1024),
    )(*arrays)


def call(
    node_latents, edge_latents, targets, edge_weight_in, edge_weight_out, node_weight_in, node_weight_out,
    readout_weight, send_rows, far_rows, edge_sender, edge_receiver, edge_count, land_mask, lat_band,
):
    nodes, width = node_latents.shape[1:]
    edges = edge_latents.shape[1]
    variables = targets.shape[2]
    patches, reps = lax.axis_size("patch"), lax.axis_size("rep")
    slot = send_rows.shape[1] // 6
    far = far_rows.shape[1] // patches
    near = 6 * slot
    remote_rows = near + patches * far
    ext = -(-(nodes + remote_rows) // 16) * 16
    tile = edges
    share = width // patches
    vmem = pl.BlockSpec(memory_space=pltpu.VMEM)
    hbm = pl.BlockSpec(memory_space=pltpu.HBM)
    dma = lambda n: pltpu.SemaphoreType.DMA((n,))
    args = (
        node_latents[0], edge_latents[0], targets[0], edge_weight_in, edge_weight_out, node_weight_in,
        node_weight_out, readout_weight, send_rows, far_rows, edge_sender, edge_receiver, edge_count,
        land_mask, lat_band)
    scratch = [(pltpu.SMEM if i == 12 else pltpu.VMEM)(a.shape, a.dtype) for i, a in enumerate(args)] + [dma(len(args))]
    scratch += [
        pltpu.VMEM((6, slot, width), BF16), pltpu.VMEM((6, slot, width), BF16),
        pltpu.VMEM((patches, far, width), BF16), pltpu.VMEM((patches, far, width), BF16),
        pltpu.VMEM((6, slot, width), BF16), pltpu.VMEM((6, slot, width), BF16),
        pltpu.VMEM((patches, far, width), BF16), pltpu.VMEM((patches, far, width), BF16),
        pltpu.VMEM((ext, width), BF16),
        pltpu.VMEM((ext + nodes, width), BF16),
        pltpu.VMEM((ext + nodes, edges), BF16),
        pltpu.VMEM((edges, width), F32),
        pltpu.VMEM((edges, width), BF16),
        pltpu.VMEM((edges, width), BF16),
        pltpu.VMEM((edges, 1), F32),
        pltpu.VMEM((edges, width), BF16),
        pltpu.VMEM((edges, width), BF16),
        pltpu.VMEM((nodes, width), BF16),
        pltpu.VMEM((nodes, width), F32),
        pltpu.VMEM((ext, width), BF16),
        pltpu.VMEM((nodes, width), BF16),
        pltpu.VMEM((nodes, width), F32),
        pltpu.VMEM((nodes, variables), F32),
        dma(4), dma(4),
    ]
    sizes = {"side": 2, "wide": reps // 2, "low": 2, "high": patches // 2}
    for _, kind, rows, columns, _ in stream_specs(share, width, variables):
        scratch += stream_scratch(kind, rows, columns, sizes)
    shape = pltpu.VMEM
    args = tuple(a if i == 12 else pltpu.with_memory_space_constraint(a, pltpu.HBM) for i, a in enumerate(args))
    outs = pl.pallas_call(
        functools.partial(kernel, (patches, reps, slot, far, ext, tile)),
        out_shape=(
            shape((nodes, width), BF16), shape((edges, width), BF16),
            shape((3 * share, width), F32), shape((share, width), F32),
            shape((2 * share, width), F32), shape((share, width), F32), shape((share, variables), F32),
        ),
        in_specs=[hbm] * len(args),
        out_specs=tuple([vmem] * 7),
        scratch_shapes=scratch,
        compiler_params=pltpu.CompilerParams(
            collective_id=0, has_side_effects=True, vmem_limit_bytes=40 * 1024 * 1024),
    )(*args)
    outs = settle(outs)
    return (outs[0][None], outs[1][None]) + tuple(outs[2:])


def solution(mesh):
    rows = P("rep", "patch", None)
    in_specs = (rows,) * 3 + (P(),) * 5 + (P("patch", None),) * 2 + (P("patch"),) * 5
    out_specs = (rows,) * 2 + (P("patch", None),) * 5
    return jax.shard_map(call, mesh=mesh, in_specs=in_specs, out_specs=out_specs, check_vma=False)
```

```python
import functools

import jax
import jax.numpy as jnp
from jax import lax
from jax.experimental import pallas as pl
from jax.experimental.pallas import tpu as pltpu
from jax.sharding import PartitionSpec as P

OCEAN = 32
BANDS = 721
MESH = pl.DeviceIdType.MESH
F32 = jnp.float32
BF16 = jnp.bfloat16


def mm(left, right):
    return jnp.dot(left, right, preferred_element_type=F32)


def mm_left(left, right):
    return lax.dot_general(left, right, (((0,), (0,)), ((), ())), preferred_element_type=F32)


def mm_right(left, right):
    return lax.dot_general(left, right, (((1,), (1,)), ((), ())), preferred_element_type=F32)


def logistic(values):
    return 0.5 * jnp.tanh(0.5 * values) + 0.5


def mean(values):
    return jnp.mean(values, axis=-1, keepdims=True)


def parse(kind):
    order = ("side",) + tuple(AXES[letter] for letter in kind if letter in AXES)
    return order, "W" in kind, "+" in kind


AXES = {"l": "low", "w": "wide", "h": "high"}


class Stream:
    def __init__(self, refs, kind, sizes, patch, rep):
        self.sizes, self.patch, self.rep = sizes, patch, rep
        self.order, self.sums, self.direct = parse(kind)
        n = len(self.order)
        self.own, self.got, self.acc = refs[0], refs[1 : 1 + n], refs[1 + n : 1 + 2 * n]
        self.last, self.fin, self.send, self.recv = refs[1 + 2 * n :]
        self.at = {"side": lax.rem(rep, 2), "wide": lax.div(rep, 2), "low": lax.rem(patch, 2), "high": lax.div(patch, 2)}
        self.sent, self.wait, self.done = None, None, 0

    def device(self, axis, index):
        at = dict(self.at)
        at[axis] = index
        return (2 * at["high"] + at["low"], 2 * at["wide"] + at["side"])

    def others(self, axis):
        size = self.sizes[axis]
        return [(d, lax.rem(self.at[axis] + d, size)) for d in range(1, size)]

    def peers(self, axis):
        return [self.device(axis, other) for _, other in self.others(axis)]

    def launch(self, ids, pairs, whole):
        if self.sent is not None:
            self.sent()
        copies = []
        for device, (src, dst) in zip(ids, pairs):
            copies.append(pltpu.make_async_remote_copy(
                src_ref=src, dst_ref=dst, send_sem=self.send.at[0], recv_sem=self.recv.at[self.done - 1],
                device_id=device, device_id_type=MESH))
            copies[-1].start()
        if len(copies) == 1:
            self.sent, self.wait = copies[0].wait_send, copies[0].wait_recv
        else:
            self.sent = pltpu.make_async_copy(whole, whole, self.send.at[0]).wait
            self.wait = pltpu.make_async_copy(whole, whole, self.recv.at[self.done - 1]).wait

    def arrive(self):
        if self.wait is not None:
            self.wait()
        self.wait = None

    def total(self, first, rest, count):
        if count == 1:
            return first + rest[0]
        value = first.astype(F32)
        for d in range(count):
            value = value + rest[d].astype(F32)
        return value.astype(BF16)

    def step(self):
        now, stages = self.done, len(self.order)
        self.done += 1
        held = self.own
        self.arrive()
        self.complete = now == stages + (1 if self.direct else 2)
        if self.complete:
            return
        if 0 < now <= stages:
            axis = self.order[now - 1]
            before = self.own if now == 1 else self.acc[now - 2]
            held = self.acc[now - 1]
            held[...] = self.total(before[self.at[axis]], self.got[now - 1], self.sizes[axis] - 1)
        if now < stages:
            axis = self.order[now]
            pairs = [(held.at[other], self.got[now].at[d - 1]) for d, other in self.others(axis)]
            self.launch(self.peers(axis), pairs, self.got[now])
            return
        side, wide = self.at["side"], self.at["wide"]
        if self.direct:
            self.fin[side, wide] = held[...]
            reps = self.sizes["side"] * self.sizes["wide"]
            ids = [(self.patch, lax.rem(self.rep + d, reps)) for d in range(1, reps)]
            self.launch(ids, [(held, self.fin.at[side, wide])] * (reps - 1), self.last)
            return
        if now == stages:
            if not self.sums:
                self.fin[side, wide] = held[...]
            pairs = [
                (held, self.last.at[d - 1] if self.sums else self.fin.at[side, wide])
                for d, _ in self.others("wide")]
            self.launch(self.peers("wide"), pairs, self.last)
        elif now == stages + 1:
            if self.sums:
                self.fin[side] = self.total(self.acc[-1][...], self.last, self.sizes["wide"] - 1)
            self.launch(self.peers("side"), [(self.fin.at[side], self.fin.at[side])], None)

    def finish(self):
        self.sent()


def stream_scratch(kind, rows, width, sizes):
    order, sums, direct = parse(kind)
    lead = tuple(sizes[a] for a in order)
    scratch = [pltpu.VMEM(lead + (rows, width), BF16)]
    for i, axis in enumerate(order):
        scratch.append(pltpu.VMEM((max(sizes[axis] - 1, 1),) + lead[i + 1 :] + (rows, width), BF16))
    for i in range(len(order)):
        scratch.append(pltpu.VMEM(lead[i + 1 :] + (rows, width), BF16))
    last = sizes["side"] * sizes["wide"] - 1 if direct else max(sizes["wide"] - 1, 1)
    scratch.append(pltpu.VMEM((last, rows, width), BF16))
    fin = (sizes["side"],) if sums and not direct else (sizes["side"], sizes["wide"])
    scratch.append(pltpu.VMEM(fin + (rows, width), BF16))
    return scratch + [pltpu.SemaphoreType.DMA((1,)), pltpu.SemaphoreType.DMA((len(order) + (1 if direct else 2),))]


def layout(stream, block):
    rows, width = stream.own.shape[-2:]
    by_row = block["by_row"]
    wides = 1 if stream.sums else stream.sizes["wide"]
    for side in range(2):
        for wide in range(wides):
            low = block["low"] + wide * rows + (side * rows * wides if by_row else 0)
            col = block["col"] + (0 if by_row else side * width)
            yield side, wide, low, col, rows, width


def put(stream, value, block):
    patches = stream.sizes["low"] * stream.sizes["high"]
    height = value.shape[0] // patches
    for p in range(patches):
        for side, wide, low, col, rows, width in layout(stream, block):
            at = {"side": side, "wide": wide, "low": p % 2, "high": p // 2}
            stream.own[tuple(at[a] for a in stream.order) + (slice(None), slice(None))] = value[
                p * height + low : p * height + low + rows, col : col + width
            ].astype(BF16)


def take(stream, out, block, scale, shift=0):
    for side, wide, low, col, rows, width in layout(stream, block):
        if stream.sums and stream.direct:
            held = stream.fin[side, 0].astype(F32)
            for w in range(1, stream.sizes["wide"]):
                held = held + stream.fin[side, w].astype(F32)
        else:
            held = (stream.fin[side] if stream.sums else stream.fin[side, wide]).astype(F32)
        out[low : low + rows, shift + col : shift + col + width] = held * scale


def stream_specs(share, width, variables):
    sides = {
        "ro": (share, variables), "no": (share, width), "ni": (2 * share, width), "eo": (share, width),
        "c0": (3 * share, width // 2), "c1": (3 * share, width // 2)}
    specs = []
    for group, down, across, kinds in STREAMS:
        height, columns = sides[group][0] // down, sides[group][1] // across
        by_row = group == "ro"
        for i, kind in enumerate(kinds):
            rows, cols = (height // 2, columns) if by_row else (height, columns // 2)
            place = {"low": (i // across) * height, "col": (i % across) * columns, "by_row": by_row}
            specs.append((f"{group}_{i}", kind, rows if parse(kind)[1] else rows // 2, cols, place))
    return specs


def kernel(
    dims,
    x_h, e_h, tgt_h, wein_h, weout_h, wnin_h, wnout_h, wro_h, send_h, far_h, es_h, er_h, count_h, land_h, lat_h,
    o_node, o_edge, o_ein, o_eout, o_nin, o_nout, o_ro,
    x, e, tgt, w_ein, w_eout, w_nin, w_nout, w_ro, send_ids, far_ids, es, er, count, land, lat, loaded,
    near_out, near_in, far_out, far_in, back_near_out, back_near_in, back_far_out, back_far_in,
    xext, xw, table, sgrad, hid, msg, inv, ezg, epg, agg_grad, total, sums, rsums, local, loss_weight,
    aggregate, node_hidden, z_grad, updated, pred_grad, up_grad, node_sgrad,
    halo_sems, back_sems,
    *stream_refs,
):
    patches, reps, slot, far, ext, tile = dims
    nodes, width = x.shape
    edges = e.shape[0]
    near = 6 * slot
    share = width // patches
    half = width // 2
    patch, rep = lax.axis_index("patch"), lax.axis_index("rep")
    sizes = {"side": 2, "wide": reps // 2, "low": 2, "high": patches // 2}

    barrier = pltpu.get_barrier_semaphore()
    for d in range(1, patches):
        pl.semaphore_signal(barrier, inc=1, device_id=(lax.rem(patch + d, patches), rep), device_id_type=MESH)
    for d in range(1, reps):
        pl.semaphore_signal(barrier, inc=1, device_id=(patch, lax.rem(rep + d, reps)), device_id_type=MESH)

    loads = {}
    order = ("x", "send", "far", "wein", "er", "es", "count", "e", "weout", "wnin", "wnout", "wro", "tgt", "land", "lat")
    source = dict(
        x=(x_h, x), send=(send_h, send_ids), far=(far_h, far_ids), wein=(wein_h, w_ein), er=(er_h, er), es=(es_h, es),
        count=(count_h, count), e=(e_h, e), weout=(weout_h, w_eout), wnin=(wnin_h, w_nin), wnout=(wnout_h, w_nout),
        wro=(wro_h, w_ro), tgt=(tgt_h, tgt), land=(land_h, land), lat=(lat_h, lat))
    for i, name in enumerate(order):
        loads[name] = pltpu.make_async_copy(source[name][0], source[name][1], loaded.at[i])
        loads[name].start()

    specs = stream_specs(share, width, tgt.shape[1])
    streams, used = [], 0
    for _, kind, _, _, _ in specs:
        refs = 5 + 2 * len(parse(kind)[0])
        streams.append(Stream(stream_refs[used : used + refs], kind, sizes, patch, rep))
        used += refs
    named = {spec[0]: s for s, spec in zip(streams, specs)}
    groups = {}
    for s, spec in zip(streams, specs):
        groups.setdefault(spec[0][:2], []).append((s, spec[4]))

    def put_group(group, value):
        for s, place in groups[group]:
            put(s, value, place)
            s.step()

    returned = []

    def send_back():
        for k in range(6):
            back_near_out[k] = sums[nodes + k * slot : nodes + (k + 1) * slot, :]
        for q in range(patches):
            low = nodes + near + q * far
            back_far_out[q] = sums[low : low + far, :]
        returned.extend(exchange(-1, back_near_out, back_near_in, back_far_out, back_far_in, back_sems))

    def node_out():
        for c in returned[1]:
            c.wait()
        near_back = jnp.concatenate([back_near_in[k] for k in range(6)], axis=0)
        far_back = jnp.concatenate([back_far_in[q].astype(F32) for q in range(patches)], axis=0).astype(BF16)
        owned = mm(own_near, near_back) + mm(own_far, far_back)
        owned = (owned + local[...]).astype(BF16)
        o_node[...] = (total[...] + mm_right(owned, w_s[...])).astype(BF16)

    scale = 1.0 / (nodes * patches * reps)
    into = {"ro": (o_ro, 0), "no": (o_nout, 0), "ni": (o_nin, 0), "eo": (o_eout, 0), "c0": (o_ein, 0), "c1": (o_ein, half)}
    places = {spec[0]: spec[4] for spec in specs}
    actions = {"back": send_back, "node": node_out}
    plan = iter(PLAN)

    def tick():
        for name in next(plan):
            if name in actions:
                actions[name]()
                continue
            named[name].step()
            if named[name].complete:
                out, shift = into[name[:2]]
                take(named[name], out, places[name], scale, shift)

    def listed(ids):
        hit = lax.broadcasted_iota(jnp.int32, (nodes, ids.shape[1]), 0) == ids[...]
        return jnp.where(hit, 1.0, 0.0).astype(BF16)

    for name in ("x", "send", "far"):
        loads[name].wait()
    own_near, own_far = listed(send_ids), listed(far_ids)
    outgoing, outgoing_far = mm_left(own_near, x[...]), mm_left(own_far, x[...])
    for k in range(6):
        near_out[k] = outgoing[k * slot : (k + 1) * slot].astype(BF16)
    for q in range(patches):
        far_out[q] = outgoing_far[q * far : (q + 1) * far].astype(BF16)
    pl.semaphore_wait(barrier, patches - 1 + reps - 1)

    def remote(src, dst, send, recv, device):
        c = pltpu.make_async_remote_copy(
            src_ref=src, dst_ref=dst, send_sem=send, recv_sem=recv, device_id=device, device_id_type=MESH)
        c.start()
        return c

    def exchange(sign, near_from, near_to, far_from, far_to, sems):
        near_send, near_recv, far_send, far_recv = (sems.at[i] for i in range(4))
        for d in range(1, patches):
            to = lax.rem(patch + d, patches)
            remote(far_from.at[to], far_to.at[patch], far_send, far_recv, (to, rep))
        upper = lax.div(patch, patches // 2)
        if sign < 0:
            upper = 1 - upper
        for m, down in ((1, 1), (2, 1), (3, 1), (3, 0), (2, 0), (1, 0)):
            down = 1 - upper if down else upper
            k = 2 * (m - 1) + down
            to = lax.rem(patch + sign * m * (1 - 2 * down) + patches, patches)
            remote(near_from.at[k], near_to.at[k], near_send, near_recv, (to, rep))
        far_to[patch] = far_from[patch]
        others = far_from.at[pl.ds(0, patches - 1)]
        return (
            [pltpu.make_async_copy(near_from, near_from, near_send), pltpu.make_async_copy(others, others, far_send)],
            [pltpu.make_async_copy(near_to, near_to, near_recv), pltpu.make_async_copy(others, others, far_recv)])

    halo_sent, halo = exchange(1, near_out, near_in, far_out, far_in, halo_sems)

    w_s, w_r, w_e = (w_ein.at[pl.ds(i * width, width)] for i in range(3))
    loads["wein"].wait()
    xext[0:nodes, :] = x[...]
    xw[0:nodes, :] = mm(x[...], w_s[...]).astype(BF16)
    xw[nodes : 2 * nodes, :] = mm(x[...], w_r[...]).astype(BF16)
    own, far_rows = 2 * nodes, ext - nodes

    for name in ("er", "es", "count", "e"):
        loads[name].wait()

    def tables(t):
        at = slice(t * tile, (t + 1) * tile)
        ids = es[at][None, :]
        hit = lax.broadcasted_iota(jnp.int32, (nodes, tile), 0) == ids
        table[0:nodes, at] = jnp.where(hit, 1.0, 0.0).astype(BF16)
        hit = lax.broadcasted_iota(jnp.int32, (far_rows, tile), 0) + nodes == ids
        table[own : own + far_rows, at] = jnp.where(hit, 1.0, 0.0).astype(BF16)
        alive = lax.broadcasted_iota(jnp.int32, (1, tile), 1) + t * tile < count[0]
        ids = jnp.where(alive, er[at][None, :], -1)
        hit = lax.broadcasted_iota(jnp.int32, (nodes, tile), 0) == ids
        table[nodes : 2 * nodes, at] = jnp.where(hit, 1.0, 0.0).astype(BF16)

    def edge_local(t):
        at = slice(t * tile, (t + 1) * tile)
        sgrad[at, :] = mm(e[at, :], w_e[...]) + mm_left(table[0:own, at], xw[0:own, :])

    parts = range(edges // tile)
    for t in parts:
        tables(t)
        edge_local(t)

    for name in order[8:]:
        loads[name].wait()
    variables = tgt.shape[1]
    latitude = -0.5 * jnp.pi + (lat[...].astype(F32) + 0.5) * (jnp.pi / BANDS)
    area = jnp.broadcast_to(jnp.cos(latitude)[None, :], (variables, nodes))
    ocean = lax.broadcasted_iota(jnp.int32, (variables, nodes), 0) < OCEAN
    masked = jnp.broadcast_to((land[...])[None, :], (variables, nodes)) == 1
    loss_weight[...] = jnp.transpose(jnp.where(ocean & masked, 0.0, area))
    total[...] = mm(x[...], w_nin[0:width, :])

    for c in halo:
        c.wait()
    pieces = [near_in[k] for k in range(6)] + [far_in[q] for q in range(patches)]
    pad = ext - nodes - near - patches * far
    if pad:
        pieces.append(jnp.zeros((pad, width), BF16))
    arrived = jnp.concatenate([v.astype(F32) for v in pieces], axis=0).astype(BF16)
    xext[nodes:ext, :] = arrived
    xw[own : own + far_rows, :] = mm(arrived, w_s[...]).astype(BF16)

    def edge_hidden(t):
        at = slice(t * edges // 2, (t + 1) * edges // 2)
        pre = sgrad[at, :] + mm_left(table[own : own + far_rows, at], xw[own : own + far_rows, :])
        s = logistic(pre)
        h = pre * s
        sgrad[at, :] = s + h * (1.0 - s)
        hid[at, :] = h.astype(BF16)

    def edge_normed(t):
        at = slice(t * edges // 2, (t + 1) * edges // 2)
        z = mm(hid[at, :], w_eout[...])
        centred = z - mean(z)
        inverse = lax.rsqrt(mean(centred * centred) + 1e-05)
        inv[at, :] = inverse
        msg[at, :] = (centred * inverse).astype(BF16)

    for t in range(2):
        edge_hidden(t)
    for t in range(2):
        edge_normed(t)

    aggregate[...] = mm(table[nodes : 2 * nodes, :], msg[...]).astype(BF16)

    def node_part(low, high):
        at = slice(low, high)
        node_pre = total[at, :] + mm(aggregate[at, :], w_nin[width : 2 * width, :])
        s = logistic(node_pre)
        h = node_pre * s
        node_hidden[at, :] = h.astype(BF16)
        node_sgrad[at, :] = s + h * (1.0 - s)
        yield
        z = mm(node_hidden[at, :], w_nout[...])
        centred = z - mean(z)
        inverse = lax.rsqrt(mean(centred * centred) + 1e-05)
        normed = centred * inverse
        updated[at, :] = (x[at, :].astype(F32) + normed).astype(BF16)
        yield
        pred_grad[at, :] = (loss_weight[at, :] * (mm(updated[at, :], w_ro[...]) - tgt[at, :].astype(F32))).astype(BF16)
        yield
        up = mm_right(pred_grad[at, :], w_ro[...])
        up_grad[at, :] = up
        z_grad[at, :] = (inverse * (up - mean(up) - normed * mean(up * normed))).astype(BF16)
        yield

    node_parts = [node_part(0, nodes // 2), node_part(nodes // 2, nodes)]
    for _ in range(4):
        for part in node_parts:
            next(part)
    put_group("no", mm_left(node_hidden[...], z_grad[...]))
    tick()
    pre_grad = (mm_right(z_grad[...], w_nout[...]) * node_sgrad[...]).astype(BF16)
    put_group("ni", jnp.concatenate([mm_left(x[...], pre_grad), mm_left(aggregate[...], pre_grad)], axis=0))
    tick()
    total[...] = up_grad[...] + mm_right(pre_grad, w_nin[0:width, :])
    message_grad = mm_right(pre_grad, w_nin[width : 2 * width, :])
    agg_grad[...] = (message_grad - mean(message_grad)).astype(BF16)
    put_group("ro", mm_left(updated[...], pred_grad[...]))
    tick()

    def edge_backward(t):
        at = slice(t * edges // 2, (t + 1) * edges // 2)
        g = mm_left(table[nodes : 2 * nodes, at], agg_grad[...])
        y = msg[at, :].astype(F32)
        zg = (inv[at, :] * (g - y * mean(g * y))).astype(BF16)
        ezg[at, :] = zg
        epg[at, :] = (mm_right(zg, w_eout[...]) * sgrad[at, :]).astype(BF16)

    for t in range(2):
        edge_backward(t)
        tick()
    put_group("eo", mm_left(hid[...], ezg[...]))
    tick()

    for c, group in enumerate(("c0", "c1")):
        at = pl.ds(c * half, half)
        sums32 = mm(table[0:nodes, :], epg[:, at])
        local[:, at] = sums32
        sums[0:nodes, at] = sums32.astype(BF16)
        sums[nodes:ext, at] = mm(table[own : own + far_rows, :], epg[:, at]).astype(BF16)
        tick()
        rsums[:, at] = mm(table[nodes : 2 * nodes, :], epg[:, at]).astype(BF16)
        tick()
        first = mm_left(e[...], epg[:, at])
        tick()
        put_group(group, jnp.concatenate(
            [mm_left(xext[...], sums[:, at]), mm_left(x[...], rsums[:, at]), first], axis=0))
        tick()

    for t in range(2):
        at = slice(t * edges // 2, (t + 1) * edges // 2)
        o_edge[at, :] = mm_right(epg[at, :], w_e[...]).astype(BF16)
        tick()
    total[...] += mm_right(rsums[...], w_r[...])
    tick()
    assert all(s.complete for s in streams)
    for c in halo_sent + returned[0]:
        c.wait()
    for s in streams:
        s.finish()


STREAMS = (
    ("ro", 1, 1, ("wlh",)),
    ("no", 1, 2, ("lwh+", "wlh")),
    ("ni", 1, 2, ("hlw+", "lwh")),
    ("eo", 1, 2, ("wlh+", "wlh+")),
    ("c0", 2, 1, ("lwh+", "wlh")),
    ("c1", 3, 1, ("hlW+", "lwh+", "wlh+")),
)


PLAN = (
    (),
    (),
    ("no_0", "no_1"),
    ("ni_0",),
    ("ni_1", "ro_0"),
    (),
    ("no_0", "no_1"),
    (),
    ("eo_0",),
    ("eo_1", "ro_0"),
    ("back",),
    (),
    ("no_0", "c0_0", "ni_1"),
    ("c0_1", "no_1"),
    ("ro_0", "eo_0"),
    (),
    ("c1_0", "ni_0", "eo_1", "c1_1", "c1_2", "ni_1", "node", "c0_0", "no_0", "eo_0", "no_1", "c0_1", "ro_0",
     "ni_0", "eo_1", "c1_2", "c1_1", "c0_0", "no_0", "c1_0", "no_1", "ro_0", "c0_1", "ni_0", "no_1", "ro_0",
     "c1_2", "ni_1", "eo_0", "c1_1", "c1_0", "eo_1", "ni_0", "c0_0", "ni_1", "eo_0", "c0_1", "ni_1", "c1_0",
     "c1_2", "eo_1", "c1_1", "c0_0", "c0_1", "c1_2", "c0_1", "c1_1"),
)


def settle_kernel(n, *refs):
    src, dst, sem = refs[:n], refs[n : 2 * n], refs[2 * n]
    copies = [pltpu.make_async_copy(src[i], dst[i], sem.at[i]) for i in range(n)]
    for c in copies:
        c.start()
    for c in copies:
        c.wait()


def settle(arrays):
    n = len(arrays)
    return pl.pallas_call(
        functools.partial(settle_kernel, n),
        out_shape=tuple(jax.ShapeDtypeStruct(a.shape, a.dtype) for a in arrays),
        in_specs=[pl.BlockSpec(memory_space=pltpu.VMEM)] * n,
        out_specs=tuple([pl.BlockSpec(memory_space=pltpu.HBM)] * n),
        scratch_shapes=[pltpu.SemaphoreType.DMA((n,))],
        compiler_params=pltpu.CompilerParams(vmem_limit_bytes=4 * 1024 * 1024),
    )(*arrays)


def call(
    node_latents, edge_latents, targets, edge_weight_in, edge_weight_out, node_weight_in, node_weight_out,
    readout_weight, send_rows, far_rows, edge_sender, edge_receiver, edge_count, land_mask, lat_band,
):
    nodes, width = node_latents.shape[1:]
    edges = edge_latents.shape[1]
    variables = targets.shape[2]
    patches, reps = lax.axis_size("patch"), lax.axis_size("rep")
    slot = send_rows.shape[1] // 6
    far = far_rows.shape[1] // patches
    near = 6 * slot
    remote_rows = near + patches * far
    ext = -(-(nodes + remote_rows) // 16) * 16
    tile = edges
    share = width // patches
    vmem = pl.BlockSpec(memory_space=pltpu.VMEM)
    hbm = pl.BlockSpec(memory_space=pltpu.HBM)
    dma = lambda n: pltpu.SemaphoreType.DMA((n,))
    args = (
        node_latents[0], edge_latents[0], targets[0], edge_weight_in, edge_weight_out, node_weight_in,
        node_weight_out, readout_weight, send_rows, far_rows, edge_sender, edge_receiver, edge_count,
        land_mask, lat_band)
    scratch = [(pltpu.SMEM if i == 12 else pltpu.VMEM)(a.shape, a.dtype) for i, a in enumerate(args)] + [dma(len(args))]
    scratch += [
        pltpu.VMEM((6, slot, width), BF16), pltpu.VMEM((6, slot, width), BF16),
        pltpu.VMEM((patches, far, width), BF16), pltpu.VMEM((patches, far, width), BF16),
        pltpu.VMEM((6, slot, width), BF16), pltpu.VMEM((6, slot, width), BF16),
        pltpu.VMEM((patches, far, width), BF16), pltpu.VMEM((patches, far, width), BF16),
        pltpu.VMEM((ext, width), BF16),
        pltpu.VMEM((ext + nodes, width), BF16),
        pltpu.VMEM((ext + nodes, edges), BF16),
        pltpu.VMEM((edges, width), F32),
        pltpu.VMEM((edges, width), BF16),
        pltpu.VMEM((edges, width), BF16),
        pltpu.VMEM((edges, 1), F32),
        pltpu.VMEM((edges, width), BF16),
        pltpu.VMEM((edges, width), BF16),
        pltpu.VMEM((nodes, width), BF16),
        pltpu.VMEM((nodes, width), F32),
        pltpu.VMEM((ext, width), BF16),
        pltpu.VMEM((nodes, width), BF16),
        pltpu.VMEM((nodes, width), F32),
        pltpu.VMEM((nodes, variables), F32),
        *[pltpu.VMEM((nodes, width), BF16)] * 4, pltpu.VMEM((nodes, variables), BF16),
        *[pltpu.VMEM((nodes, width), F32)] * 2,
        dma(4), dma(4),
    ]
    sizes = {"side": 2, "wide": reps // 2, "low": 2, "high": patches // 2}
    for _, kind, rows, columns, _ in stream_specs(share, width, variables):
        scratch += stream_scratch(kind, rows, columns, sizes)
    shape = pltpu.VMEM
    args = tuple(a if i == 12 else pltpu.with_memory_space_constraint(a, pltpu.HBM) for i, a in enumerate(args))
    outs = pl.pallas_call(
        functools.partial(kernel, (patches, reps, slot, far, ext, tile)),
        out_shape=(
            shape((nodes, width), BF16), shape((edges, width), BF16),
            shape((3 * share, width), F32), shape((share, width), F32),
            shape((2 * share, width), F32), shape((share, width), F32), shape((share, variables), F32),
        ),
        in_specs=[hbm] * len(args),
        out_specs=tuple([vmem] * 7),
        scratch_shapes=scratch,
        compiler_params=pltpu.CompilerParams(
            collective_id=0, has_side_effects=True, vmem_limit_bytes=40 * 1024 * 1024),
    )(*args)
    outs = settle(outs)
    return (outs[0][None], outs[1][None]) + tuple(outs[2:])


def solution(mesh):
    rows = P("rep", "patch", None)
    in_specs = (rows,) * 3 + (P(),) * 5 + (P("patch", None),) * 2 + (P("patch"),) * 5
    out_specs = (rows,) * 2 + (P("patch", None),) * 5
    return jax.shard_map(call, mesh=mesh, in_specs=in_specs, out_specs=out_specs, check_vma=False)
```

```python
import functools

import jax
import jax.numpy as jnp
from jax import lax
from jax.experimental import pallas as pl
from jax.experimental.pallas import tpu as pltpu
from jax.sharding import PartitionSpec as P

OCEAN = 32
BANDS = 721
MESH = pl.DeviceIdType.MESH
F32 = jnp.float32
BF16 = jnp.bfloat16


def mm(left, right):
    return jnp.dot(left, right, preferred_element_type=F32)


def mm_left(left, right):
    return lax.dot_general(left, right, (((0,), (0,)), ((), ())), preferred_element_type=F32)


def mm_right(left, right):
    return lax.dot_general(left, right, (((1,), (1,)), ((), ())), preferred_element_type=F32)


def logistic(values):
    return 0.5 * jnp.tanh(0.5 * values) + 0.5


def mean(values):
    return jnp.mean(values, axis=-1, keepdims=True)


def parse(kind):
    order = ("side",) + tuple(AXES[letter] for letter in kind if letter in AXES)
    return order, "W" in kind, "+" in kind


AXES = {"l": "low", "w": "wide", "h": "high"}


class Stream:
    def __init__(self, refs, kind, sizes, patch, rep):
        self.sizes, self.patch, self.rep = sizes, patch, rep
        self.order, self.sums, self.direct = parse(kind)
        n = len(self.order)
        self.own, self.got, self.acc = refs[0], refs[1 : 1 + n], refs[1 + n : 1 + 2 * n]
        self.last, self.fin, self.send, self.recv = refs[1 + 2 * n :]
        self.at = {"side": lax.rem(rep, 2), "wide": lax.div(rep, 2), "low": lax.rem(patch, 2), "high": lax.div(patch, 2)}
        self.sent, self.wait, self.done = None, None, 0

    def device(self, axis, index):
        at = dict(self.at)
        at[axis] = index
        return (2 * at["high"] + at["low"], 2 * at["wide"] + at["side"])

    def others(self, axis):
        size = self.sizes[axis]
        return [(d, lax.rem(self.at[axis] + d, size)) for d in range(1, size)]

    def peers(self, axis):
        return [self.device(axis, other) for _, other in self.others(axis)]

    def launch(self, ids, pairs, whole):
        if self.sent is not None:
            self.sent()
        copies = []
        for device, (src, dst) in zip(ids, pairs):
            copies.append(pltpu.make_async_remote_copy(
                src_ref=src, dst_ref=dst, send_sem=self.send.at[0], recv_sem=self.recv.at[self.done - 1],
                device_id=device, device_id_type=MESH))
            copies[-1].start()
        if len(copies) == 1:
            self.sent, self.wait = copies[0].wait_send, copies[0].wait_recv
        else:
            self.sent = pltpu.make_async_copy(whole, whole, self.send.at[0]).wait
            self.wait = pltpu.make_async_copy(whole, whole, self.recv.at[self.done - 1]).wait

    def arrive(self):
        if self.wait is not None:
            self.wait()
        self.wait = None

    def total(self, first, rest, count):
        if count == 1:
            return first + rest[0]
        value = first.astype(F32)
        for d in range(count):
            value = value + rest[d].astype(F32)
        return value.astype(BF16)

    def step(self):
        now, stages = self.done, len(self.order)
        self.done += 1
        held = self.own
        self.arrive()
        self.complete = now == stages + (1 if self.direct else 2)
        if self.complete:
            return
        if 0 < now <= stages:
            axis = self.order[now - 1]
            before = self.own if now == 1 else self.acc[now - 2]
            held = self.acc[now - 1]
            held[...] = self.total(before[self.at[axis]], self.got[now - 1], self.sizes[axis] - 1)
        if now < stages:
            axis = self.order[now]
            pairs = [(held.at[other], self.got[now].at[d - 1]) for d, other in self.others(axis)]
            self.launch(self.peers(axis), pairs, self.got[now])
            return
        side, wide = self.at["side"], self.at["wide"]
        if self.direct:
            self.fin[side, wide] = held[...]
            reps = self.sizes["side"] * self.sizes["wide"]
            ids = [(self.patch, lax.rem(self.rep + d, reps)) for d in range(1, reps)]
            self.launch(ids, [(held, self.fin.at[side, wide])] * (reps - 1), self.last)
            return
        if now == stages:
            if not self.sums:
                self.fin[side, wide] = held[...]
            pairs = [
                (held, self.last.at[d - 1] if self.sums else self.fin.at[side, wide])
                for d, _ in self.others("wide")]
            self.launch(self.peers("wide"), pairs, self.last)
        elif now == stages + 1:
            if self.sums:
                self.fin[side] = self.total(self.acc[-1][...], self.last, self.sizes["wide"] - 1)
            self.launch(self.peers("side"), [(self.fin.at[side], self.fin.at[side])], None)

    def finish(self):
        self.sent()


def stream_scratch(kind, rows, width, sizes):
    order, sums, direct = parse(kind)
    lead = tuple(sizes[a] for a in order)
    scratch = [pltpu.VMEM(lead + (rows, width), BF16)]
    for i, axis in enumerate(order):
        scratch.append(pltpu.VMEM((max(sizes[axis] - 1, 1),) + lead[i + 1 :] + (rows, width), BF16))
    for i in range(len(order)):
        scratch.append(pltpu.VMEM(lead[i + 1 :] + (rows, width), BF16))
    last = sizes["side"] * sizes["wide"] - 1 if direct else max(sizes["wide"] - 1, 1)
    scratch.append(pltpu.VMEM((last, rows, width), BF16))
    fin = (sizes["side"],) if sums and not direct else (sizes["side"], sizes["wide"])
    scratch.append(pltpu.VMEM(fin + (rows, width), BF16))
    return scratch + [pltpu.SemaphoreType.DMA((1,)), pltpu.SemaphoreType.DMA((len(order) + (1 if direct else 2),))]


def layout(stream, block):
    rows, width = stream.own.shape[-2:]
    by_row = block["by_row"]
    wides = 1 if stream.sums else stream.sizes["wide"]
    for side in range(2):
        for wide in range(wides):
            low = block["low"] + wide * rows + (side * rows * wides if by_row else 0)
            col = block["col"] + (0 if by_row else side * width)
            yield side, wide, low, col, rows, width


def put(stream, value, block):
    patches = stream.sizes["low"] * stream.sizes["high"]
    height = value.shape[0] // patches
    for p in range(patches):
        for side, wide, low, col, rows, width in layout(stream, block):
            at = {"side": side, "wide": wide, "low": p % 2, "high": p // 2}
            stream.own[tuple(at[a] for a in stream.order) + (slice(None), slice(None))] = value[
                p * height + low : p * height + low + rows, col : col + width
            ].astype(BF16)


def take(stream, out, block, scale, shift=0):
    for side, wide, low, col, rows, width in layout(stream, block):
        if stream.sums and stream.direct:
            held = stream.fin[side, 0].astype(F32)
            for w in range(1, stream.sizes["wide"]):
                held = held + stream.fin[side, w].astype(F32)
        else:
            held = (stream.fin[side] if stream.sums else stream.fin[side, wide]).astype(F32)
        out[low : low + rows, shift + col : shift + col + width] = held * scale


def stream_specs(share, width, variables):
    sides = {
        "ro": (share, variables), "no": (share, width), "ni": (2 * share, width), "eo": (share, width),
        "c0": (3 * share, width // 2), "c1": (3 * share, width // 2)}
    specs = []
    for group, down, across, kinds in STREAMS:
        height, columns = sides[group][0] // down, sides[group][1] // across
        by_row = group == "ro"
        for i, kind in enumerate(kinds):
            rows, cols = (height // 2, columns) if by_row else (height, columns // 2)
            place = {"low": (i // across) * height, "col": (i % across) * columns, "by_row": by_row}
            specs.append((f"{group}_{i}", kind, rows if parse(kind)[1] else rows // 2, cols, place))
    return specs


def kernel(
    dims,
    x_h, e_h, tgt_h, wein_h, weout_h, wnin_h, wnout_h, wro_h, send_h, far_h, es_h, er_h, count_h, land_h, lat_h,
    o_node, o_edge, o_ein, o_eout, o_nin, o_nout, o_ro,
    x, e, tgt, w_ein, w_eout, w_nin, w_nout, w_ro, send_ids, far_ids, es, er, count, land, lat, loaded,
    near_out, near_in, far_out, far_in, back_near_out, back_near_in, back_far_out, back_far_in,
    xext, xw, table, sgrad, hid, msg, inv, ezg, epg, agg_grad, total, sums, rsums, local, loss_weight,
    aggregate, node_hidden, z_grad, updated, pred_grad, up_grad, node_sgrad,
    halo_sems, back_sems,
    *stream_refs,
):
    patches, reps, slot, far, ext, tile = dims
    nodes, width = x.shape
    edges = e.shape[0]
    near = 6 * slot
    share = width // patches
    half = width // 2
    patch, rep = lax.axis_index("patch"), lax.axis_index("rep")
    sizes = {"side": 2, "wide": reps // 2, "low": 2, "high": patches // 2}

    barrier = pltpu.get_barrier_semaphore()
    for d in range(1, patches):
        pl.semaphore_signal(barrier, inc=1, device_id=(lax.rem(patch + d, patches), rep), device_id_type=MESH)
    for d in range(1, reps):
        pl.semaphore_signal(barrier, inc=1, device_id=(patch, lax.rem(rep + d, reps)), device_id_type=MESH)

    loads = {}
    order = ("x", "send", "far", "wein", "er", "es", "count", "e", "weout", "wnin", "wnout", "wro", "tgt", "land", "lat")
    source = dict(
        x=(x_h, x), send=(send_h, send_ids), far=(far_h, far_ids), wein=(wein_h, w_ein), er=(er_h, er), es=(es_h, es),
        count=(count_h, count), e=(e_h, e), weout=(weout_h, w_eout), wnin=(wnin_h, w_nin), wnout=(wnout_h, w_nout),
        wro=(wro_h, w_ro), tgt=(tgt_h, tgt), land=(land_h, land), lat=(lat_h, lat))
    for i, name in enumerate(order):
        loads[name] = pltpu.make_async_copy(source[name][0], source[name][1], loaded.at[i])
        loads[name].start()

    specs = stream_specs(share, width, tgt.shape[1])
    streams, used = [], 0
    for _, kind, _, _, _ in specs:
        refs = 5 + 2 * len(parse(kind)[0])
        streams.append(Stream(stream_refs[used : used + refs], kind, sizes, patch, rep))
        used += refs
    named = {spec[0]: s for s, spec in zip(streams, specs)}
    groups = {}
    for s, spec in zip(streams, specs):
        groups.setdefault(spec[0][:2], []).append((s, spec[4]))

    def put_group(group, value):
        for s, place in groups[group]:
            put(s, value, place)
            s.step()

    returned = []

    def send_back():
        for k in range(6):
            back_near_out[k] = sums[nodes + k * slot : nodes + (k + 1) * slot, :]
        for q in range(patches):
            low = nodes + near + q * far
            back_far_out[q] = sums[low : low + far, :]
        returned.extend(exchange(-1, back_near_out, back_near_in, back_far_out, back_far_in, back_sems))

    def node_out():
        for c in returned[1]:
            c.wait()
        near_back = jnp.concatenate([back_near_in[k] for k in range(6)], axis=0)
        far_back = jnp.concatenate([back_far_in[q].astype(F32) for q in range(patches)], axis=0).astype(BF16)
        owned = mm(own_near, near_back) + mm(own_far, far_back)
        owned = (owned + local[...]).astype(BF16)
        o_node[...] = (total[...] + mm_right(owned, w_s[...])).astype(BF16)

    scale = 1.0 / (nodes * patches * reps)
    into = {"ro": (o_ro, 0), "no": (o_nout, 0), "ni": (o_nin, 0), "eo": (o_eout, 0), "c0": (o_ein, 0), "c1": (o_ein, half)}
    places = {spec[0]: spec[4] for spec in specs}
    actions = {"back": send_back, "node": node_out}
    plan = iter(PLAN)

    def tick():
        for name in next(plan):
            if name in actions:
                actions[name]()
                continue
            named[name].step()
            if named[name].complete:
                out, shift = into[name[:2]]
                take(named[name], out, places[name], scale, shift)

    def listed(ids):
        hit = lax.broadcasted_iota(jnp.int32, (nodes, ids.shape[1]), 0) == ids[...]
        return jnp.where(hit, 1.0, 0.0).astype(BF16)

    for name in ("x", "send", "far"):
        loads[name].wait()
    own_near, own_far = listed(send_ids), listed(far_ids)
    outgoing, outgoing_far = mm_left(own_near, x[...]), mm_left(own_far, x[...])
    for k in range(6):
        near_out[k] = outgoing[k * slot : (k + 1) * slot].astype(BF16)
    for q in range(patches):
        far_out[q] = outgoing_far[q * far : (q + 1) * far].astype(BF16)
    pl.semaphore_wait(barrier, patches - 1 + reps - 1)

    def remote(src, dst, send, recv, device):
        c = pltpu.make_async_remote_copy(
            src_ref=src, dst_ref=dst, send_sem=send, recv_sem=recv, device_id=device, device_id_type=MESH)
        c.start()
        return c

    def exchange(sign, near_from, near_to, far_from, far_to, sems):
        near_send, near_recv, far_send, far_recv = (sems.at[i] for i in range(4))
        for d in range(1, patches):
            to = lax.rem(patch + d, patches)
            remote(far_from.at[to], far_to.at[patch], far_send, far_recv, (to, rep))
        upper = lax.div(patch, patches // 2)
        if sign < 0:
            upper = 1 - upper
        for m, down in ((1, 1), (2, 1), (3, 1), (3, 0), (2, 0), (1, 0)):
            down = 1 - upper if down else upper
            k = 2 * (m - 1) + down
            to = lax.rem(patch + sign * m * (1 - 2 * down) + patches, patches)
            remote(near_from.at[k], near_to.at[k], near_send, near_recv, (to, rep))
        far_to[patch] = far_from[patch]
        others = far_from.at[pl.ds(0, patches - 1)]
        return (
            [pltpu.make_async_copy(near_from, near_from, near_send), pltpu.make_async_copy(others, others, far_send)],
            [pltpu.make_async_copy(near_to, near_to, near_recv), pltpu.make_async_copy(others, others, far_recv)])

    halo_sent, halo = exchange(1, near_out, near_in, far_out, far_in, halo_sems)

    w_s, w_r, w_e = (w_ein.at[pl.ds(i * width, width)] for i in range(3))
    loads["wein"].wait()
    xext[0:nodes, :] = x[...]
    xw[0:nodes, :] = mm(x[...], w_s[...]).astype(BF16)
    xw[nodes : 2 * nodes, :] = mm(x[...], w_r[...]).astype(BF16)
    own, far_rows = 2 * nodes, ext - nodes

    for name in ("er", "es", "count", "e"):
        loads[name].wait()

    def tables(t):
        at = slice(t * tile, (t + 1) * tile)
        ids = es[at][None, :]
        hit = lax.broadcasted_iota(jnp.int32, (nodes, tile), 0) == ids
        table[0:nodes, at] = jnp.where(hit, 1.0, 0.0).astype(BF16)
        hit = lax.broadcasted_iota(jnp.int32, (far_rows, tile), 0) + nodes == ids
        table[own : own + far_rows, at] = jnp.where(hit, 1.0, 0.0).astype(BF16)
        alive = lax.broadcasted_iota(jnp.int32, (1, tile), 1) + t * tile < count[0]
        ids = jnp.where(alive, er[at][None, :], -1)
        hit = lax.broadcasted_iota(jnp.int32, (nodes, tile), 0) == ids
        table[nodes : 2 * nodes, at] = jnp.where(hit, 1.0, 0.0).astype(BF16)

    def edge_local(t):
        at = slice(t * tile, (t + 1) * tile)
        sgrad[at, :] = mm(e[at, :], w_e[...]) + mm_left(table[0:own, at], xw[0:own, :])

    parts = range(edges // tile)
    for t in parts:
        tables(t)
        edge_local(t)

    for name in order[8:]:
        loads[name].wait()
    variables = tgt.shape[1]
    latitude = -0.5 * jnp.pi + (lat[...].astype(F32) + 0.5) * (jnp.pi / BANDS)
    area = jnp.broadcast_to(jnp.cos(latitude)[None, :], (variables, nodes))
    ocean = lax.broadcasted_iota(jnp.int32, (variables, nodes), 0) < OCEAN
    masked = jnp.broadcast_to((land[...])[None, :], (variables, nodes)) == 1
    loss_weight[...] = jnp.transpose(jnp.where(ocean & masked, 0.0, area))
    total[...] = mm(x[...], w_nin[0:width, :])

    for c in halo:
        c.wait()
    pieces = [near_in[k] for k in range(6)] + [far_in[q] for q in range(patches)]
    pad = ext - nodes - near - patches * far
    if pad:
        pieces.append(jnp.zeros((pad, width), BF16))
    arrived = jnp.concatenate([v.astype(F32) for v in pieces], axis=0).astype(BF16)
    xext[nodes:ext, :] = arrived
    xw[own : own + far_rows, :] = mm(arrived, w_s[...]).astype(BF16)

    def edge_hidden(t):
        at = slice(t * edges // 2, (t + 1) * edges // 2)
        pre = sgrad[at, :] + mm_left(table[own : own + far_rows, at], xw[own : own + far_rows, :])
        s = logistic(pre)
        h = pre * s
        sgrad[at, :] = s + h * (1.0 - s)
        hid[at, :] = h.astype(BF16)

    def edge_normed(t):
        at = slice(t * edges // 2, (t + 1) * edges // 2)
        z = mm(hid[at, :], w_eout[...])
        centred = z - mean(z)
        inverse = lax.rsqrt(mean(centred * centred) + 1e-05)
        inv[at, :] = inverse
        msg[at, :] = (centred * inverse).astype(BF16)

    for t in range(2):
        edge_hidden(t)
    for t in range(2):
        edge_normed(t)

    aggregate[...] = mm(table[nodes : 2 * nodes, :], msg[...]).astype(BF16)

    def node_part(low, high):
        at = slice(low, high)
        node_pre = total[at, :] + mm(aggregate[at, :], w_nin[width : 2 * width, :])
        s = logistic(node_pre)
        h = node_pre * s
        node_hidden[at, :] = h.astype(BF16)
        node_sgrad[at, :] = s + h * (1.0 - s)
        yield
        z = mm(node_hidden[at, :], w_nout[...])
        centred = z - mean(z)
        inverse = lax.rsqrt(mean(centred * centred) + 1e-05)
        normed = centred * inverse
        updated[at, :] = (x[at, :].astype(F32) + normed).astype(BF16)
        yield
        pred_grad[at, :] = (loss_weight[at, :] * (mm(updated[at, :], w_ro[...]) - tgt[at, :].astype(F32))).astype(BF16)
        yield
        up = mm_right(pred_grad[at, :], w_ro[...])
        up_grad[at, :] = up
        z_grad[at, :] = (inverse * (up - mean(up) - normed * mean(up * normed))).astype(BF16)
        yield

    node_parts = [node_part(0, nodes // 2), node_part(nodes // 2, nodes)]
    for _ in range(4):
        for part in node_parts:
            next(part)
    put_group("no", mm_left(node_hidden[...], z_grad[...]))
    tick()
    pre_grad = (mm_right(z_grad[...], w_nout[...]) * node_sgrad[...]).astype(BF16)
    put_group("ni", jnp.concatenate([mm_left(x[...], pre_grad), mm_left(aggregate[...], pre_grad)], axis=0))
    tick()
    total[...] = up_grad[...] + mm_right(pre_grad, w_nin[0:width, :])
    message_grad = mm_right(pre_grad, w_nin[width : 2 * width, :])
    agg_grad[...] = (message_grad - mean(message_grad)).astype(BF16)
    put_group("ro", mm_left(updated[...], pred_grad[...]))
    tick()

    def edge_backward(t):
        at = slice(t * edges // 2, (t + 1) * edges // 2)
        g = mm_left(table[nodes : 2 * nodes, at], agg_grad[...])
        y = msg[at, :].astype(F32)
        zg = (inv[at, :] * (g - y * mean(g * y))).astype(BF16)
        ezg[at, :] = zg
        epg[at, :] = (mm_right(zg, w_eout[...]) * sgrad[at, :]).astype(BF16)

    for t in range(2):
        edge_backward(t)
        tick()
    put_group("eo", mm_left(hid[...], ezg[...]))
    tick()

    for c, group in enumerate(("c0", "c1")):
        at = pl.ds(c * half, half)
        sums32 = mm(table[0:nodes, :], epg[:, at])
        local[:, at] = sums32
        sums[0:nodes, at] = sums32.astype(BF16)
        sums[nodes:ext, at] = mm(table[own : own + far_rows, :], epg[:, at]).astype(BF16)
        tick()
        rsums[:, at] = mm(table[nodes : 2 * nodes, :], epg[:, at]).astype(BF16)
        tick()
        first = mm_left(e[...], epg[:, at])
        tick()
        put_group(group, jnp.concatenate(
            [mm_left(xext[...], sums[:, at]), mm_left(x[...], rsums[:, at]), first], axis=0))
        tick()

    for t in range(2):
        at = slice(t * edges // 2, (t + 1) * edges // 2)
        o_edge[at, :] = mm_right(epg[at, :], w_e[...]).astype(BF16)
        tick()
    total[...] += mm_right(rsums[...], w_r[...])
    tick()
    assert all(s.complete for s in streams)
    for c in halo_sent + returned[0]:
        c.wait()
    for s in streams:
        s.finish()


STREAMS = (
    ("ro", 1, 1, ("wlh",)),
    ("no", 1, 2, ("lwh+", "wlh")),
    ("ni", 1, 2, ("hlW", "lwh")),
    ("eo", 1, 2, ("wlh+", "wlh")),
    ("c0", 2, 1, ("lwh+", "wlh")),
    ("c1", 3, 1, ("hlw", "wlh+", "lwh+")),
)


PLAN = (
    (),
    (),
    ("no_0", "no_1"),
    ("ni_0",),
    ("ni_1", "ro_0"),
    (),
    ("no_0", "no_1"),
    (),
    ("eo_0",),
    ("eo_1", "ro_0"),
    ("back",),
    (),
    ("no_0", "c0_0", "ni_1"),
    ("c0_1", "no_1"),
    ("ro_0", "eo_0"),
    (),
    ("c1_0", "ni_0", "eo_1", "c1_1", "c1_2", "ni_1", "node", "c0_0", "no_0", "eo_0", "no_1", "c0_1", "ro_0",
     "ni_0", "eo_1", "c1_1", "c1_2", "c0_0", "no_0", "c1_0", "no_1", "ro_0", "c0_1", "ni_0", "no_1", "ro_0",
     "c1_1", "ni_1", "ni_0", "eo_0", "c1_2", "c1_0", "eo_1", "c0_0", "ni_1", "eo_0", "c0_1", "c1_0", "ni_1",
     "eo_1", "c1_1", "c1_2", "eo_1", "c0_0", "c0_1", "c1_0", "c1_1", "c0_1", "c1_0", "c1_2"),
)


def settle_kernel(n, *refs):
    src, dst, sem = refs[:n], refs[n : 2 * n], refs[2 * n]
    copies = [pltpu.make_async_copy(src[i], dst[i], sem.at[i]) for i in range(n)]
    for c in copies:
        c.start()
    for c in copies:
        c.wait()


def settle(arrays):
    n = len(arrays)
    return pl.pallas_call(
        functools.partial(settle_kernel, n),
        out_shape=tuple(jax.ShapeDtypeStruct(a.shape, a.dtype) for a in arrays),
        in_specs=[pl.BlockSpec(memory_space=pltpu.VMEM)] * n,
        out_specs=tuple([pl.BlockSpec(memory_space=pltpu.HBM)] * n),
        scratch_shapes=[pltpu.SemaphoreType.DMA((n,))],
        compiler_params=pltpu.CompilerParams(vmem_limit_bytes=4 * 1024 * 1024),
    )(*arrays)


def call(
    node_latents, edge_latents, targets, edge_weight_in, edge_weight_out, node_weight_in, node_weight_out,
    readout_weight, send_rows, far_rows, edge_sender, edge_receiver, edge_count, land_mask, lat_band,
):
    nodes, width = node_latents.shape[1:]
    edges = edge_latents.shape[1]
    variables = targets.shape[2]
    patches, reps = lax.axis_size("patch"), lax.axis_size("rep")
    slot = send_rows.shape[1] // 6
    far = far_rows.shape[1] // patches
    near = 6 * slot
    remote_rows = near + patches * far
    ext = -(-(nodes + remote_rows) // 16) * 16
    tile = edges
    share = width // patches
    vmem = pl.BlockSpec(memory_space=pltpu.VMEM)
    hbm = pl.BlockSpec(memory_space=pltpu.HBM)
    dma = lambda n: pltpu.SemaphoreType.DMA((n,))
    args = (
        node_latents[0], edge_latents[0], targets[0], edge_weight_in, edge_weight_out, node_weight_in,
        node_weight_out, readout_weight, send_rows, far_rows, edge_sender, edge_receiver, edge_count,
        land_mask, lat_band)
    scratch = [(pltpu.SMEM if i == 12 else pltpu.VMEM)(a.shape, a.dtype) for i, a in enumerate(args)] + [dma(len(args))]
    scratch += [
        pltpu.VMEM((6, slot, width), BF16), pltpu.VMEM((6, slot, width), BF16),
        pltpu.VMEM((patches, far, width), BF16), pltpu.VMEM((patches, far, width), BF16),
        pltpu.VMEM((6, slot, width), BF16), pltpu.VMEM((6, slot, width), BF16),
        pltpu.VMEM((patches, far, width), BF16), pltpu.VMEM((patches, far, width), BF16),
        pltpu.VMEM((ext, width), BF16),
        pltpu.VMEM((ext + nodes, width), BF16),
        pltpu.VMEM((ext + nodes, edges), BF16),
        pltpu.VMEM((edges, width), F32),
        pltpu.VMEM((edges, width), BF16),
        pltpu.VMEM((edges, width), BF16),
        pltpu.VMEM((edges, 1), F32),
        pltpu.VMEM((edges, width), BF16),
        pltpu.VMEM((edges, width), BF16),
        pltpu.VMEM((nodes, width), BF16),
        pltpu.VMEM((nodes, width), F32),
        pltpu.VMEM((ext, width), BF16),
        pltpu.VMEM((nodes, width), BF16),
        pltpu.VMEM((nodes, width), F32),
        pltpu.VMEM((nodes, variables), F32),
        *[pltpu.VMEM((nodes, width), BF16)] * 4, pltpu.VMEM((nodes, variables), BF16),
        *[pltpu.VMEM((nodes, width), F32)] * 2,
        dma(4), dma(4),
    ]
    sizes = {"side": 2, "wide": reps // 2, "low": 2, "high": patches // 2}
    for _, kind, rows, columns, _ in stream_specs(share, width, variables):
        scratch += stream_scratch(kind, rows, columns, sizes)
    shape = pltpu.VMEM
    args = tuple(a if i == 12 else pltpu.with_memory_space_constraint(a, pltpu.HBM) for i, a in enumerate(args))
    outs = pl.pallas_call(
        functools.partial(kernel, (patches, reps, slot, far, ext, tile)),
        out_shape=(
            shape((nodes, width), BF16), shape((edges, width), BF16),
            shape((3 * share, width), F32), shape((share, width), F32),
            shape((2 * share, width), F32), shape((share, width), F32), shape((share, variables), F32),
        ),
        in_specs=[hbm] * len(args),
        out_specs=tuple([vmem] * 7),
        scratch_shapes=scratch,
        compiler_params=pltpu.CompilerParams(
            collective_id=0, has_side_effects=True, vmem_limit_bytes=40 * 1024 * 1024),
    )(*args)
    outs = settle(outs)
    return (outs[0][None], outs[1][None]) + tuple(outs[2:])


def solution(mesh):
    rows = P("rep", "patch", None)
    in_specs = (rows,) * 3 + (P(),) * 5 + (P("patch", None),) * 2 + (P("patch"),) * 5
    out_specs = (rows,) * 2 + (P("patch", None),) * 5
    return jax.shard_map(call, mesh=mesh, in_specs=in_specs, out_specs=out_specs, check_vma=False)
```
